32 devices in a mesh: tm: 4 (over z), batch: 4 (over x, core), width: 2 (over y).
Axes of the slice: x: 2, y: 2, z: 4, core: 2. Of those that a mesh axis runs over, the one named last changes fastest.
Arguments:
- moves: int32 [8, 1024], P('batch', 'tm'), may hold values from 0 to 361
- lengths: int32 [8], P('batch'), may hold values from 1 to 1024
- outcomes: int32 [8], P('batch'), may hold values from -1 to 1
- embedded: bfloat16 [8, 1024, 2048], P('batch', 'tm', 'width'), may hold values from -6 to 6
- w_branches: bfloat16 [4, 2048, 2048], P(None, ('tm', 'batch'), 'width'), may hold values from -0.125 to 0.125
- conv_w: float32 [4, 2048], P(None, 'width'), may hold values from -3 to 3
- gate_bias: float32 [2, 2048], P(None, 'width'), may hold values from -4 to 4
- rates: float32 [2048], P('width'), may hold values from 0.001 to 0.105
- w_down: bfloat16 [2048, 2048], P(('tm', 'batch'), 'width'), may hold values from -0.125 to 0.125
- w_policy: bfloat16 [2048, 362], P('width'), may hold values from -12 to 12
- w_value: bfloat16 [2048], P('width'), may hold values from -0.125 to 0.125
Outputs:
- position_loss: float32 [8, 1024], P('batch', 'tm')
- value: float32 [8, 1024], P('batch', 'tm')
The draws below stay inside these ranges and needn't reach their ends.
All inputs are finite; a program needn't handle non-finite values.
Results may differ from the reference program's by a relative error of at most 0.0033.
Values may be sent and summed in bfloat16 or wider, within the bound.
A program may use at most 128 MiB of HBM per device.

```python
import math
import jax
import jax.numpy as jnp
from jax import lax

D = 2048
R = 2048
MOVES = 362
KERNEL = 4
GAMES = 8
TIME = 1024


def draw_w_policy(key, part):
    first = jax.random.fold_in(jax.random.fold_in(key, 17), 0)
    base = jax.random.normal(first, (D, MOVES), jnp.float32) / math.sqrt(D)
    return jnp.clip(base, -12.0, 12.0).astype(jnp.bfloat16)


def set_ends(values, rng, least, largest):
    longest = values.shape.index(max(values.shape))
    spots = []
    for shift in (0, 1):
        where = [jax.random.randint(jax.random.fold_in(rng, axis), (), 0, length) for axis, length in enumerate(values.shape)]
        where[longest] = (where[longest] + shift) % values.shape[longest]
        spots.append(tuple(where))
    return values.at[spots[0]].set(least).at[spots[1]].set(largest)


def shard_levels(rng, dims, cuts, least, top_value):
    def one(axis_at, shards_of):
        steps = jax.random.uniform(jax.random.fold_in(jax.random.fold_in(rng, 6), axis_at), (shards_of,), jnp.float32, least / len(cuts), top_value / len(cuts))
        return jnp.repeat(jnp.exp(steps), dims[axis_at] // shards_of).reshape((-1,) + (1,) * (len(dims) - axis_at - 1))

    level = one(*cuts[0])
    for cut in cuts[1:]:
        level = level * one(*cut)
    return level


def gaussian(stream_key, extent, deviation, reach, cuts=(), kind=jnp.bfloat16):
    level = shard_levels(stream_key, extent, cuts, -0.22, 0.18) if cuts else 1.0
    entries = jax.random.normal(stream_key, extent, jnp.float32) * deviation * level
    return jnp.minimum(jnp.maximum(entries, -reach), reach).astype(kind)


def setup_inputs(seed: int = 0) -> dict:
    key_list = jax.random.split(jax.random.key(seed), 12)
    moves = set_ends(jax.random.randint(key_list[0], (GAMES, TIME), 0, MOVES), jax.random.fold_in(key_list[0], 1), 0, MOVES - 1).astype(jnp.int32)
    lengths = set_ends(jax.random.randint(key_list[1], (GAMES,), 1, TIME + 1), jax.random.fold_in(key_list[1], 1), 1, TIME).astype(jnp.int32)
    outcomes = set_ends(jax.random.randint(key_list[2], (GAMES,), -1, 2), jax.random.fold_in(key_list[2], 1), -1, 1).astype(jnp.int32)
    embedded = gaussian(key_list[3], (GAMES, TIME, D), 1.0, 6.0, ((0, 4), (1, 4), (2, 2)))
    w_branches = gaussian(key_list[4], (4, D, R), D ** -0.5, 0.125, ((1, 16), (2, 2)))
    conv_w = gaussian(key_list[5], (KERNEL, R), 0.5, 3.0, ((1, 2),), jnp.float32)
    gate_bias = gaussian(key_list[6], (2, R), 1.0, 4.0, ((1, 2),), jnp.float32)
    rates = jnp.clip(jnp.exp(math.log(0.105) - 4.65396 * jax.random.uniform(key_list[7], (R,), jnp.float32) ** shard_levels(key_list[7], (R,), ((0, 2),), -0.2, 0.2)), 0.001, 0.105)
    w_down = gaussian(key_list[8], (D, R), R ** -0.5, 0.125, ((0, 16), (1, 2)))
    w_policy = draw_w_policy(jax.random.fold_in(key_list[11], 71), 0)
    w_value = gaussian(key_list[10], (D,), D ** -0.5, 0.125, ((0, 2),))
    return {"moves": moves, "lengths": lengths, "outcomes": outcomes, "embedded": embedded, "w_branches": w_branches, "conv_w": conv_w, "gate_bias": gate_bias, "rates": rates, "w_down": w_down, "w_policy": w_policy, "w_value": w_value}


def link(early, late):
    return (early[0] + late[0], jnp.exp(late[0]) * early[1] + late[1])

def reference(moves, lengths, outcomes, embedded, w_branches, conv_w, gate_bias, rates, w_down, w_policy, w_value):

    def one_game(packed):
        feats, played, length, result = packed
        proj = [jnp.dot(feats, w_branches[k], preferred_element_type=jnp.float32) for k in range(4)]
        gated = jax.nn.gelu(proj[0])
        padded = jnp.concatenate([jnp.zeros((KERNEL - 1, R), jnp.float32), proj[1]], 0)
        conv = jnp.zeros((TIME, R), jnp.float32)
        for k in range(KERNEL):
            conv = conv + conv_w[k] * padded[KERNEL - 1 - k:KERNEL - 1 - k + TIME]
        recur = jax.nn.sigmoid(proj[2] + gate_bias[0])
        inflow = jax.nn.sigmoid(proj[3] + gate_bias[1])
        log_a = -8.0 * recur * rates
        decay = jnp.exp(log_a)
        drive = jnp.sqrt(1.0 - decay * decay) * inflow * conv
        summed, hidden = lax.associative_scan(link, (log_a, drive), axis=0)
        mixed = (hidden * gated).astype(jnp.bfloat16)
        down = lax.dot_general(mixed, w_down, (((1,), (1,)), ((), ())), preferred_element_type=jnp.float32)
        resid = (feats.astype(jnp.float32) + down).astype(jnp.bfloat16)
        wide = resid.astype(jnp.float32)
        sumsq = lax.optimization_barrier(jnp.sum(wide * wide, -1))
        norm = lax.rsqrt(sumsq / D + 1e-06)
        logits = jnp.dot(resid, w_policy, preferred_element_type=jnp.float32) * norm[:, None]
        value = jnp.tanh(jnp.dot(resid, w_value, preferred_element_type=jnp.float32) * norm)
        top = lax.optimization_barrier(jnp.max(logits, -1, keepdims=True))
        lse = top[:, 0] + jnp.log(lax.optimization_barrier(jnp.sum(jnp.exp(logits - top), -1)))
        column = lax.broadcasted_iota(jnp.int32, (TIME, MOVES), 1)
        picked = lax.optimization_barrier(jnp.sum(jnp.where(column == played[:, None], logits, 0.0), -1))
        target = result.astype(jnp.float32)
        where_live = jnp.arange(TIME, dtype=jnp.int32) < length
        loss = jnp.where(where_live, lse - picked + (value - target) ** 2, 0.0)
        return (loss, value)
    return lax.map(one_game, (embedded, moves, lengths, outcomes))
```

```python
import jax
import jax.numpy as jnp
from jax import lax
from jax.experimental import pallas as pl
from jax.experimental.pallas import tpu as pltpu
from jax.sharding import PartitionSpec as P

KERNEL = 4
SUB = 8
LANE = 128
MESH = pl.DeviceIdType.MESH
DIRS = (0, 1)
PAIRS = (0, 1)


def core_kernel(
    emb, wb, wd, heads_in, wval, conv_w, bias, rates, moves, lengths, outcomes,
    out_loss, out_value,
    w_all, wd_all, raw, feat, tail_buf, tails, acc, carry_s, ends, mix, mix_in, down, heads, wval_all, res,
    loc_w, loc_d, loc_e, loc_h, feat_s, feat_r, tail_s, tail_r, val_s, val_r, head_s, head_r, hrel_s, hrel_r,
    ring_s, ring_r, peer_s, peer_r, dring_s, dring_r, dpeer_s, dpeer_r, dpart_s, dpart_r, drel_s, drel_r,
    ends_s, ends_r, mix_s, mix_r, res_s, res_r,
):
    z, b, y = lax.axis_index("tm"), lax.axis_index("batch"), lax.axis_index("width")
    zn, bn, yn = lax.axis_size("tm"), lax.axis_size("batch"), lax.axis_size("width")
    x, core = b // 2, b % 2
    n = zn * (bn // 2)
    rows, chans = wd.shape
    games, steps, half = emb.shape
    depth = yn * half
    count = games * steps
    seg = steps // SUB
    chunks = chans // LANE
    wide = 2 * LANE
    items = chans // wide
    reach = n // 2
    per = n // 4
    other = yn - 1 - y

    def spot(r):
        cx = r // zn
        cz = r % zn
        return cz + (cx % 2) * (zn - 1 - 2 * cz), cx

    r = x * zn + z + (x % 2) * (zn - 1 - 2 * z)

    def at(place, c=core, w=y):
        return {"tm": place[0], "batch": place[1] * 2 + c, "width": w}

    ahead, behind = at(spot((r + 1) % n)), at(spot((r + n - 1) % n))
    peer = at((z, x), 1 - core)
    partner = at((z, x), core, other)
    after = ((z + 1) % zn, x)
    before = ((z + zn - 1) % zn, x)
    greet = [ahead, behind, peer, partner, at(after), at(after, core, other), at(before), at(before, core, other)]
    greet += [at(((z + d) % zn, x)) for d in range(2, zn - 1)]

    def first_row(chip):
        cz, cx = spot(chip)
        return (cz * bn + cx * 2) * rows

    def block(chip, c):
        return pl.ds(pl.multiple_of(first_row(chip) + c * rows, rows), rows)

    mine = block(r, core)

    def remote(src, dst, send, recv, device):
        return pltpu.make_async_remote_copy(
            src_ref=src, dst_ref=dst, send_sem=send, recv_sem=recv, device_id=device, device_id_type=MESH
        )

    def load_chunk(c):
        return [
            pltpu.make_async_copy(
                wb.at[m, :, pl.ds(pl.multiple_of(c * LANE, LANE), LANE)],
                w_all.at[c, m // 2, mine, (m % 2) * LANE : (m % 2 + 1) * LANE],
                loc_w.at[c],
            )
            for m in range(4)
        ]

    own_emb = pltpu.make_async_copy(emb, raw.at[y], loc_e)
    own_heads = pltpu.make_async_copy(heads_in, heads.at[pl.ds(pl.multiple_of(y * half, half), half), :], loc_h)
    for copy in load_chunk(0):
        copy.start()
    own_emb.start()
    for c in range(1, chunks):
        for copy in load_chunk(c):
            copy.start()
    for j in range(items):
        pltpu.make_async_copy(wd.at[:, j * wide : (j + 1) * wide], wd_all.at[j, y, mine, :], loc_d.at[j]).start()
    own_heads.start()
    ends[...] = jnp.zeros_like(ends)
    res[...] = jnp.zeros_like(res)
    wval_all[y] = wval[...]
    barrier = pltpu.get_barrier_semaphore()
    for device in greet:
        pl.semaphore_signal(barrier, inc=1, device_id=device, device_id_type=MESH)
    pl.semaphore_wait(barrier, len(greet))

    def chip_of(d, t):
        return (r + n - t) % n if d == 0 else (r + t) % n

    def toward(d):
        return ahead if d == 0 else behind

    def hops(which, d):
        return reach if which == d else n - 1 - reach

    def piece(c, p, chip):
        return w_all.at[c, p, block(chip, core), :]

    def hop(c, p, d, t):
        ref = piece(c, p, chip_of(d, t - 1))
        return remote(ref, ref, ring_s.at[c], ring_r.at[c, p, d, t - 1], toward(d))

    def landed(c, p, d, t):
        ref = piece(c, p, chip_of(d, t))
        return remote(ref, ref, ring_s.at[c], ring_r.at[c, p, d, t - 1], toward(d))

    def share(c, p, chip):
        ref = piece(c, p, chip)
        return remote(ref, ref, peer_s.at[c], peer_r.at[c], peer)

    def begin(c):
        ref = w_all.at[c, :, 0:rows, :]
        pltpu.make_async_copy(ref, ref, loc_w.at[c]).wait()
        for p in PAIRS:
            for d in DIRS:
                hop(c, p, d, 1).start()
        for p in PAIRS:
            share(c, p, r).start()

    def pump(c, t):
        for p, d in ((0, 0), (1, 1), (1, 0), (0, 1)):
            last = hops(p, d)

            @pl.when(t <= last)
            def _():
                landed(c, p, d, t).wait_recv()

                @pl.when(t < last)
                def _():
                    hop(c, p, d, t + 1).start()

                share(c, p, chip_of(d, t)).start()

    def dpiece(j, w, chip, c=core):
        return wd_all.at[j, w, block(chip, c), :]

    def dhop(j, d, t):
        ref = dpiece(j, y, chip_of(d, t - 1))
        return remote(ref, ref, dring_s.at[j], dring_r.at[j, d, t - 1], toward(d))

    def dlanded(j, d, t):
        ref = dpiece(j, y, chip_of(d, t))
        return remote(ref, ref, dring_s.at[j], dring_r.at[j, d, t - 1], toward(d))

    def dspread(j, chip):
        ref = dpiece(j, y, chip)
        remote(ref, ref, dpeer_s.at[j], dpeer_r.at[j], peer).start()
        remote(ref, ref, dpart_s.at[j], dpart_r.at[j, chip], partner).start()

    def dbegin(j):
        ref = wd_all.at[j, y, mine, :]
        pltpu.make_async_copy(ref, ref, loc_d.at[j]).wait()
        for d in DIRS:
            dhop(j, d, 1).start()
        dspread(j, r)

    def dpump(j, t):
        for d in DIRS:
            last = hops(j % 2, d)

            @pl.when((t >= 1) & (t <= last))
            def _():
                dlanded(j, d, t).wait_recv()

                @pl.when(t < last)
                def _():
                    dhop(j, d, t + 1).start()

                dspread(j, chip_of(d, t))

    def drelay(j, t):
        for d in DIRS:
            last = hops(j % 2, d)

            @pl.when((t >= d) & (t <= last))
            def _():
                ref = dpiece(j, other, chip_of(d, t))
                remote(ref, ref, dpart_s.at[j], dpart_r.at[j, chip_of(d, t)], partner).wait_recv()
                remote(ref, ref, drel_s.at[j], drel_r.at[j], peer).start()

    row_id = lax.broadcasted_iota(jnp.int32, (steps, steps), 0)
    lane_id = lax.broadcasted_iota(jnp.int32, (steps, steps), 1)
    spread = (row_id % SUB) * seg + row_id // SUB == lane_id

    def prepare():
        ref = raw.at[other]
        remote(ref, ref, feat_s, feat_r, partner).wait_recv()
        turn = jnp.where(spread, 1.0, 0.0).astype(jnp.bfloat16)
        for owner in range(yn):
            for g in range(games):
                feat[g * steps : (g + 1) * steps, owner * half : (owner + 1) * half] = jnp.dot(
                    turn, raw[owner, g], preferred_element_type=jnp.float32
                ).astype(jnp.bfloat16)

        @pl.when(z > 0)
        def _():
            for i in range(2):
                ref = tails.at[y if i == 0 else other]
                remote(ref, ref, tail_s.at[i], tail_r.at[i], peer).wait_recv()
            for owner in range(yn):
                feat[count : count + games * SUB, owner * half : (owner + 1) * half] = tails[owner]

        @pl.when(z == 0)
        def _():
            feat[count : count + games * SUB, :] = jnp.zeros((games * SUB, depth), jnp.bfloat16)

        down[...] = feat[pl.ds(pl.multiple_of(y * steps, steps), steps), :].astype(jnp.float32)

    def product(c):
        ref = w_all.at[c, :, 0 : n * rows, :]
        remote(ref, ref, peer_s.at[c], peer_r.at[c], peer).wait_recv()

        @pl.loop(0, 2)
        def _(p):
            acc[p] = jnp.dot(feat[...], w_all[c, p], preferred_element_type=jnp.float32)

    lo, hi = slice(0, LANE), slice(LANE, 2 * LANE)

    def lines(g, t):
        return pl.ds(pl.multiple_of(g * steps + t * SUB, SUB), SUB)

    def ends_copy(c, d, source, place):
        ref = ends.at[c, source]
        return remote(ref, ref, ends_s.at[c, d], ends_r.at[c, d], at(place))

    def scan(c):
        cut = pl.ds(pl.multiple_of(c * LANE, LANE), LANE)
        w = [conv_w[k : k + 1, cut] for k in range(KERNEL)]
        b0, b1 = bias[0:1, cut], bias[1:2, cut]
        scale = -8.0 * rates[:, cut]
        row = lax.broadcasted_iota(jnp.int32, (SUB, LANE), 0)

        def earlier(g, j):
            rolled = pltpu.roll(acc[0, lines(g, seg - j), hi], 1, 0)
            first = count + g * SUB + SUB - j
            return jnp.where(row == 0, acc[0, first : first + 1, hi], rolled)

        def step(t, state):
            new = []
            for g in range(games):
                h, p, x1, x2, x3 = state[g]
                here = lines(g, t)
                x0 = acc[0, here, hi]
                conv = w[0] * x0 + w[1] * x1 + w[2] * x2 + w[3] * x3
                recur = jax.nn.sigmoid(acc[1, here, lo] + b0)
                inflow = jax.nn.sigmoid(acc[1, here, hi] + b1)
                a = jnp.exp(recur * scale)
                h = a * h + jnp.sqrt(1.0 - a * a) * inflow * conv
                p = a * p
                acc[0, here, lo] = jax.nn.gelu(acc[0, here, lo])
                acc[1, here, lo] = h
                acc[1, here, hi] = p
                new.append((h, p, x0, x1, x2))
            return tuple(new)

        zero = jnp.zeros((SUB, LANE), jnp.float32)
        start = tuple((zero, zero + 1.0, earlier(g, 1), earlier(g, 2), earlier(g, 3)) for g in range(games))
        final = lax.fori_loop(0, seg, step, start, unroll=2)
        for g in range(games):
            h, p = final[g][:2]
            run, dec = jnp.zeros((1, LANE), jnp.float32), jnp.ones((1, LANE), jnp.float32)
            for s in range(SUB):
                carry_s[g, 0, s : s + 1, :] = run
                carry_s[g, 1, s : s + 1, :] = dec
                run = p[s : s + 1] * run + h[s : s + 1]
                dec = p[s : s + 1] * dec
            ends[c, z, 2 * g : 2 * g + 1, :] = run
            ends[c, z, 2 * g + 1 : 2 * g + 2, :] = dec
        for d in range(1, zn):

            @pl.when(z + d < zn)
            def _():
                ends_copy(c, d, z, (z + d, x)).start()

    def mix_copy(c):
        return remote(mix.at[c, other], mix_in.at[c], mix_s.at[c], mix_r.at[c], partner)

    def finish(c):
        for d in range(1, zn):

            @pl.when(z >= d)
            def _():
                ends_copy(c, d, z - d, (z - d, x)).wait_recv()

        for g in range(games):
            run = jnp.zeros((1, LANE), jnp.float32)
            for j in range(zn - 1):
                run = jnp.where(j < z, ends[c, j, 2 * g + 1 : 2 * g + 2, :] * run + ends[c, j, 2 * g : 2 * g + 1, :], run)
            enter = carry_s[g, 0] + carry_s[g, 1] * run
            enter = jnp.concatenate([enter, enter], 0)
            for i in range(steps // 16):
                here = slice(g * steps + i * 16, g * steps + (i + 1) * 16)
                value = (acc[1, here, lo] + acc[1, here, hi] * enter) * acc[0, here, lo]
                mix[c, g, i * 16 : (i + 1) * 16, :] = value.astype(jnp.bfloat16)
        mix_copy(c).start()

    def project(j):
        for c in (2 * j, 2 * j + 1):
            mix_copy(c).wait_recv()
        ref = wd_all.at[j, y, 0 : n * rows, :]
        remote(ref, ref, dpeer_s.at[j], dpeer_r.at[j], peer).wait_recv()
        remote(ref, ref, drel_s.at[j], drel_r.at[j], peer).wait_recv()
        own = jnp.concatenate([mix[2 * j, y], mix[2 * j + 1, y]], 1)
        theirs = jnp.concatenate([mix_in[2 * j], mix_in[2 * j + 1]], 1)
        part = min(512, half)

        @pl.loop(0, depth // part)
        def _(f):
            cut = pl.ds(pl.multiple_of(f * part, part), part)
            total = down[:, cut]
            for left, w in ((own, y), (theirs, other)):
                total += lax.dot_general(
                    left, wd_all[j, w, cut, :], (((1,), (1,)), ((), ())), preferred_element_type=jnp.float32
                )
            down[:, cut] = total

    begin(0)
    swap_feat = remote(emb, raw.at[y], feat_s, feat_r, partner)
    swap_feat.start()
    swap_val = remote(wval, wval_all.at[y], val_s, val_r, partner)
    swap_val.start()
    own_emb.wait()
    last = [raw[y, g, steps - 16 : steps, :].astype(jnp.float32)[16 - SUB :] for g in range(games)]
    tail_buf[...] = jnp.concatenate(last, 0).astype(jnp.bfloat16)

    def tail_copy(i):
        return remote(tail_buf, tails.at[y], tail_s.at[i], tail_r.at[i], at(after, core, y if i == 0 else other))

    @pl.when(z < zn - 1)
    def _():
        for i in range(2):
            tail_copy(i).start()

    own_heads.wait()
    quarter = half // 2

    def head_rows(w, c):
        return heads.at[pl.ds(pl.multiple_of(w * half + c * quarter, quarter), quarter), :]

    def relay_heads_wait():
        remote(head_rows(other, core), head_rows(other, core), head_s, head_r, partner).wait_recv()

    swap_heads = remote(head_rows(y, core), head_rows(y, core), head_s, head_r, partner)
    relay_heads = remote(head_rows(other, core), head_rows(other, core), hrel_s, hrel_r, peer)
    first_d = [per + j * ((chunks - 2) * per - reach) // max(items - 1, 1) for j in range(items)]

    @pl.loop(0, chunks + 4)
    def _(k):
        @pl.loop(0, per)
        def _(i):
            slot = k * per + i
            for j in range(items):

                @pl.when(slot == first_d[j])
                def _():
                    dbegin(j)

            @pl.when((i == per - 1) & (k < chunks - 1))
            def _():
                begin(k + 1)

            @pl.when((k >= 1) & (k <= chunks))
            def _():
                pump(k - 1, per + i + 1)

            @pl.when(k < chunks)
            def _():
                pump(k, i + 1)

            for j in range(items):
                t = slot - first_d[j]
                dpump(j, t)
                drelay(j, t - 1)

            @pl.when(i == 0)
            def _():
                @pl.when((k >= 3) & (k < chunks + 3))
                def _():
                    finish(k - 3)

            @pl.when((k == 2) & (i == per - 1))
            def _():
                prepare()
                swap_heads.start()

            @pl.when((k == 5) & (i == per - 1))
            def _():
                relay_heads_wait()
                relay_heads.start()

            @pl.when(((i == 0) & (k >= 3) & (k < chunks + 2)) | ((i == per - 1) & (k == 2)))
            def _():
                product(k - 2)

            @pl.when(i == per - 1)
            def _():
                @pl.when((k >= 2) & (k < chunks + 2))
                def _():
                    scan(k - 2)

                @pl.when((k >= 5) & (k % 2 == 1))
                def _():
                    project((k - 5) // 2)

    remote(head_rows(other, 1 - core), head_rows(other, 1 - core), hrel_s, hrel_r, peer).wait_recv()
    ref = wval_all.at[other]
    remote(ref, ref, val_s, val_r, partner).wait_recv()
    resid = down[...].astype(jnp.bfloat16)
    full = resid.astype(jnp.float32)
    sumsq = jnp.sum(full * full, -1, keepdims=True)
    row = jnp.concatenate([wval_all[owner, 0:1, :] for owner in range(yn)], 1)
    score = jnp.sum(full * row, -1, keepdims=True)
    norm = lax.rsqrt(sumsq / depth + 1e-06)
    logits = jnp.dot(resid, heads[...], preferred_element_type=jnp.float32) * norm
    value = jnp.tanh(score * norm)
    top = jnp.max(logits, -1, keepdims=True)
    lse = top + jnp.log(jnp.sum(jnp.exp(logits - top), -1, keepdims=True))
    played = moves[pl.ds(y, 1), :].astype(jnp.float32)
    played = jnp.sum(jnp.where(spread, played, 0.0), -1, keepdims=True)
    column = lax.broadcasted_iota(jnp.int32, logits.shape, 1).astype(jnp.float32)
    picked = jnp.sum(jnp.where(column == played, logits, 0.0), -1, keepdims=True)
    target = outcomes[y].astype(jnp.float32)
    loss = lse - picked + (value - target) ** 2
    loss = jnp.sum(jnp.where(spread, loss, 0.0), 0, keepdims=True)
    value = jnp.sum(jnp.where(spread, value, 0.0), 0, keepdims=True)
    position = z * steps + lax.broadcasted_iota(jnp.int32, (1, steps), 1)
    loss = jnp.where(position < lengths[y], loss, 0.0)
    res[y, 0:1, :] = loss
    res[y, 1:2, :] = value
    swap_res = remote(res.at[y], res.at[y], res_s, res_r, partner)
    swap_res.start()
    ref = res.at[other]
    remote(ref, ref, res_s, res_r, partner).wait_recv()
    for owner in range(yn):
        out_loss[owner : owner + 1, :] = res[owner, 0:1, :]
        out_value[owner : owner + 1, :] = res[owner, 1:2, :]

    swap_res.wait_send()
    swap_feat.wait_send()
    swap_val.wait_send()
    swap_heads.wait_send()
    relay_heads.wait_send()

    @pl.when(z < zn - 1)
    def _():
        for i in range(2):
            tail_copy(i).wait_send()

    @pl.loop(0, chunks)
    def _(c):
        ref = w_all.at[c, :, 0 : (n - 1) * rows, :]
        remote(ref, ref, ring_s.at[c], peer_r.at[c], peer).wait_send()
        ref = w_all.at[c, :, 0 : n * rows, :]
        remote(ref, ref, peer_s.at[c], peer_r.at[c], peer).wait_send()
        mix_copy(c).wait_send()
        for d in range(1, zn):

            @pl.when(z + d < zn)
            def _():
                ends_copy(c, d, z, (z + d, x)).wait_send()

    @pl.loop(0, items)
    def _(j):
        ref = wd_all.at[j, y, 0 : (n - 1) * rows, :]
        remote(ref, ref, dring_s.at[j], dpeer_r.at[j], peer).wait_send()
        ref = wd_all.at[j, y, 0 : n * rows, :]
        for sem in (dpeer_s, dpart_s, drel_s):
            remote(ref, ref, sem.at[j], dpeer_r.at[j], peer).wait_send()


def core_block(emb, wb, wd, heads, wval, conv_w, bias, rates, moves, lengths, outcomes):
    games, steps, half = emb.shape
    rows, chans = wd.shape
    yn, zn = lax.axis_size("width"), lax.axis_size("tm")
    n = zn * (lax.axis_size("batch") // 2)
    depth, count = yn * half, games * steps
    labels = heads.shape[1]
    assert games == yn and n % 4 == 0
    chunks, wide = chans // LANE, 2 * LANE
    items, reach = chans // wide, n // 2
    vmem = pl.BlockSpec(memory_space=pltpu.VMEM)
    smem = pl.BlockSpec(memory_space=pltpu.SMEM)
    hbm = pl.BlockSpec(memory_space=pl.ANY)
    dma = pltpu.SemaphoreType.DMA
    f32, b16 = jnp.float32, jnp.bfloat16
    return pl.pallas_call(
        core_kernel,
        in_specs=[hbm] * 4 + [vmem] * 5 + [smem] * 2,
        out_specs=(vmem, vmem),
        out_shape=(jax.ShapeDtypeStruct((games, steps), f32), jax.ShapeDtypeStruct((games, steps), f32)),
        scratch_shapes=[
            pltpu.VMEM((chunks, 2, depth, wide), b16),
            pltpu.VMEM((items, yn, depth, wide), b16),
            pltpu.VMEM((yn, games, steps, half), b16),
            pltpu.VMEM((count + games * SUB, depth), b16),
            pltpu.VMEM((games * SUB, half), b16),
            pltpu.VMEM((yn, games * SUB, half), b16),
            pltpu.VMEM((2, count + games * SUB, wide), f32),
            pltpu.VMEM((games, 2, SUB, LANE), f32),
            pltpu.VMEM((chunks, zn, SUB, LANE), f32),
            pltpu.VMEM((chunks, games, steps, LANE), b16),
            pltpu.VMEM((chunks, steps, LANE), b16),
            pltpu.VMEM((steps, depth), f32),
            pltpu.VMEM((depth, labels), b16),
            pltpu.VMEM((yn, SUB, half), f32),
            pltpu.VMEM((yn, SUB, steps), f32),
            dma((chunks,)), dma((items,)), dma, dma, dma, dma, dma((2,)), dma((2,)), dma, dma, dma, dma, dma, dma,
            dma((chunks,)), dma((chunks, 2, 2, reach)), dma((chunks,)), dma((chunks,)),
            dma((items,)), dma((items, 2, reach)), dma((items,)), dma((items,)),
            dma((items,)), dma((items, n)), dma((items,)), dma((items,)),
            dma((chunks, zn)), dma((chunks, zn)), dma((chunks,)), dma((chunks,)), dma, dma,
        ],
        compiler_params=pltpu.CompilerParams(
            collective_id=0, has_side_effects=True, vmem_limit_bytes=56 * 1024 * 1024
        ),
        cost_estimate=pl.CostEstimate(
            flops=8 * count * chans * depth, bytes_accessed=200_000_000, transcendentals=8 * count * chans
        ),
    )(emb, wb, wd, heads, wval, conv_w, bias, rates, moves, lengths, outcomes)


def shards(
    moves,
    lengths,
    outcomes,
    embedded,
    w_branches,
    conv_w,
    gate_bias,
    rates,
    w_down,
    w_policy,
    w_value,
):
    wval = jnp.broadcast_to(w_value.astype(jnp.float32)[None, :], (SUB, w_value.shape[0]))
    return core_block(
        embedded, w_branches, w_down, w_policy, wval, conv_w, gate_bias, rates.reshape(1, -1), moves, lengths, outcomes
    )


def solution(mesh):
    in_specs = (
        P("batch", "tm"),
        P("batch"),
        P("batch"),
        P("batch", "tm", "width"),
        P(None, ("tm", "batch"), "width"),
        P(None, "width"),
        P(None, "width"),
        P("width"),
        P(("tm", "batch"), "width"),
        P("width", None),
        P("width"),
    )
    out_specs = (P("batch", "tm"), P("batch", "tm"))
    return jax.shard_map(shards, mesh=mesh, in_specs=in_specs, out_specs=out_specs, check_vma=False)
```

```python
import jax
import jax.numpy as jnp
from jax import lax
from jax.experimental import pallas as pl
from jax.experimental.pallas import tpu as pltpu
from jax.sharding import PartitionSpec as P

KERNEL = 4
SUB = 8
LANE = 128
MESH = pl.DeviceIdType.MESH
DIRS = (0, 1)
PAIRS = (0, 1)


def core_kernel(
    emb, wb, wd, heads_in, wval, conv_w, bias, rates, moves, lengths, outcomes,
    out,
    w_all, wd_all, raw, feat, tail_buf, tails, acc, carry_s, ends, mix, mix_in, down, heads, wval_all, res,
    loc_w, loc_d, loc_e, loc_h, feat_s, feat_r, tail_s, tail_r, val_s, val_r, head_s, head_r, hrel_s, hrel_r,
    ring_s, ring_r, peer_s, peer_r, dring_s, dring_r, dpeer_s, dpeer_r, dpart_s, dpart_r, drel_s, drel_r,
    ends_s, ends_r, mix_s, mix_r, res_s, res_r,
):
    z, b, y = lax.axis_index("tm"), lax.axis_index("batch"), lax.axis_index("width")
    zn, bn, yn = lax.axis_size("tm"), lax.axis_size("batch"), lax.axis_size("width")
    x, core = b // 2, b % 2
    n = zn * (bn // 2)
    rows, chans = wd.shape
    games, steps, half = emb.shape
    depth = yn * half
    count = games * steps
    seg = steps // SUB
    chunks = chans // LANE
    wide = 2 * LANE
    items = chans // wide
    reach = n // 2
    per = n // 4
    other = yn - 1 - y

    def spot(r):
        cx = r // zn
        cz = r % zn
        return cz + (cx % 2) * (zn - 1 - 2 * cz), cx

    r = x * zn + z + (x % 2) * (zn - 1 - 2 * z)

    def at(place, c=core, w=y):
        return {"tm": place[0], "batch": place[1] * 2 + c, "width": w}

    ahead, behind = at(spot((r + 1) % n)), at(spot((r + n - 1) % n))
    peer = at((z, x), 1 - core)
    partner = at((z, x), core, other)
    after = ((z + 1) % zn, x)
    before = ((z + zn - 1) % zn, x)
    greet = [ahead, behind, peer, partner, at(after), at(after, core, other), at(before), at(before, core, other)]
    greet += [at(((z + d) % zn, x)) for d in range(2, zn - 1)]

    def first_row(chip):
        cz, cx = spot(chip)
        return (cz * bn + cx * 2) * rows

    def block(chip, c):
        return pl.ds(pl.multiple_of(first_row(chip) + c * rows, rows), rows)

    mine = block(r, core)

    def remote(src, dst, send, recv, device):
        return pltpu.make_async_remote_copy(
            src_ref=src, dst_ref=dst, send_sem=send, recv_sem=recv, device_id=device, device_id_type=MESH
        )

    def load_chunk(c):
        return [
            pltpu.make_async_copy(
                wb.at[m, :, pl.ds(pl.multiple_of(c * LANE, LANE), LANE)],
                w_all.at[c, m // 2, mine, (m % 2) * LANE : (m % 2 + 1) * LANE],
                loc_w.at[c],
            )
            for m in range(4)
        ]

    own_emb = pltpu.make_async_copy(emb, raw.at[y], loc_e)
    own_heads = pltpu.make_async_copy(heads_in, heads.at[y], loc_h)
    for copy in load_chunk(0):
        copy.start()
    own_emb.start()
    for c in range(1, chunks):
        for copy in load_chunk(c):
            copy.start()
    for j in range(items):
        pltpu.make_async_copy(wd.at[:, j * wide : (j + 1) * wide], wd_all.at[j, y, mine, :], loc_d.at[j]).start()
    own_heads.start()
    ends[...] = jnp.zeros_like(ends)
    res[...] = jnp.zeros_like(res)
    wval_all[y] = wval[...]
    barrier = pltpu.get_barrier_semaphore()
    for device in greet:
        pl.semaphore_signal(barrier, inc=1, device_id=device, device_id_type=MESH)
    pl.semaphore_wait(barrier, len(greet))

    def chip_of(d, t):
        return (r + n - t) % n if d == 0 else (r + t) % n

    def toward(d):
        return ahead if d == 0 else behind

    def hops(which, d):
        return reach if which == d else n - 1 - reach

    def piece(c, p, chip):
        return w_all.at[c, p, block(chip, core), :]

    def hop(c, p, d, t):
        ref = piece(c, p, chip_of(d, t - 1))
        return remote(ref, ref, ring_s.at[c], ring_r.at[c, p, d, t - 1], toward(d))

    def landed(c, p, d, t):
        ref = piece(c, p, chip_of(d, t))
        return remote(ref, ref, ring_s.at[c], ring_r.at[c, p, d, t - 1], toward(d))

    def share(c, p, chip):
        ref = piece(c, p, chip)
        return remote(ref, ref, peer_s.at[c], peer_r.at[c], peer)

    def begin(c):
        ref = w_all.at[c, :, 0:rows, :]
        pltpu.make_async_copy(ref, ref, loc_w.at[c]).wait()
        for p in PAIRS:
            for d in DIRS:
                hop(c, p, d, 1).start()
        for p in PAIRS:
            share(c, p, r).start()

    def pump(c, t):
        for p, d in ((0, 0), (1, 1), (1, 0), (0, 1)):
            last = hops(p, d)

            @pl.when(t <= last)
            def _():
                landed(c, p, d, t).wait_recv()

                @pl.when(t < last)
                def _():
                    hop(c, p, d, t + 1).start()

                share(c, p, chip_of(d, t)).start()

    def dpiece(j, w, chip, c=core):
        return wd_all.at[j, w, block(chip, c), :]

    def dhop(j, d, t):
        ref = dpiece(j, y, chip_of(d, t - 1))
        return remote(ref, ref, dring_s.at[j], dring_r.at[j, d, t - 1], toward(d))

    def dlanded(j, d, t):
        ref = dpiece(j, y, chip_of(d, t))
        return remote(ref, ref, dring_s.at[j], dring_r.at[j, d, t - 1], toward(d))

    def dspread(j, chip):
        ref = dpiece(j, y, chip)
        remote(ref, ref, dpeer_s.at[j], dpeer_r.at[j], peer).start()
        remote(ref, ref, dpart_s.at[j], dpart_r.at[j, chip], partner).start()

    def dbegin(j):
        ref = wd_all.at[j, y, mine, :]
        pltpu.make_async_copy(ref, ref, loc_d.at[j]).wait()
        for d in DIRS:
            dhop(j, d, 1).start()
        dspread(j, r)

    def dpump(j, t):
        for d in DIRS:
            last = hops(j % 2, d)

            @pl.when((t >= 1) & (t <= last))
            def _():
                dlanded(j, d, t).wait_recv()

                @pl.when(t < last)
                def _():
                    dhop(j, d, t + 1).start()

                dspread(j, chip_of(d, t))

    def drelay(j, t):
        for d in DIRS:
            last = hops(j % 2, d)

            @pl.when((t >= d) & (t <= last))
            def _():
                ref = dpiece(j, other, chip_of(d, t))
                remote(ref, ref, dpart_s.at[j], dpart_r.at[j, chip_of(d, t)], partner).wait_recv()
                remote(ref, ref, drel_s.at[j], drel_r.at[j], peer).start()

    row_id = lax.broadcasted_iota(jnp.int32, (steps, steps), 0)
    lane_id = lax.broadcasted_iota(jnp.int32, (steps, steps), 1)
    spread = (row_id % SUB) * seg + row_id // SUB == lane_id

    def prepare():
        ref = raw.at[other]
        remote(ref, ref, feat_s, feat_r, partner).wait_recv()
        turn = jnp.where(spread, 1.0, 0.0).astype(jnp.bfloat16)
        for owner in range(yn):
            for g in range(games):
                feat[g * steps : (g + 1) * steps, owner * half : (owner + 1) * half] = jnp.dot(
                    turn, raw[owner, g], preferred_element_type=jnp.float32
                ).astype(jnp.bfloat16)

        @pl.when(z > 0)
        def _():
            for i in range(2):
                ref = tails.at[y if i == 0 else other]
                remote(ref, ref, tail_s.at[i], tail_r.at[i], peer).wait_recv()
            for owner in range(yn):
                feat[count : count + games * SUB, owner * half : (owner + 1) * half] = tails[owner]

        @pl.when(z == 0)
        def _():
            feat[count : count + games * SUB, :] = jnp.zeros((games * SUB, depth), jnp.bfloat16)

        down[...] = feat[pl.ds(pl.multiple_of(y * steps, steps), steps), :].astype(jnp.float32)

    def product(c):
        ref = w_all.at[c, :, 0 : n * rows, :]
        remote(ref, ref, peer_s.at[c], peer_r.at[c], peer).wait_recv()

        @pl.loop(0, 2)
        def _(p):
            acc[p] = jnp.dot(feat[...], w_all[c, p], preferred_element_type=jnp.float32)

    lo, hi = slice(0, LANE), slice(LANE, 2 * LANE)

    def lines(g, t):
        return pl.ds(pl.multiple_of(g * steps + t * SUB, SUB), SUB)

    def ends_copy(c, d, source, place):
        ref = ends.at[c, source]
        return remote(ref, ref, ends_s.at[c, d], ends_r.at[c, d], at(place))

    def scan(c):
        cut = pl.ds(pl.multiple_of(c * LANE, LANE), LANE)
        w = [conv_w[k : k + 1, cut] for k in range(KERNEL)]
        b0, b1 = bias[0:1, cut], bias[1:2, cut]
        scale = -8.0 * rates[:, cut]
        row = lax.broadcasted_iota(jnp.int32, (SUB, LANE), 0)
        tall = min(64, steps)

        def earlier(g, j):
            rolled = pltpu.roll(acc[0, lines(g, seg - j), hi], 1, 0)
            first = count + g * SUB + SUB - j
            return jnp.where(row == 0, acc[0, first : first + 1, hi], rolled)

        for g in range(games):
            old = [earlier(g, j) for j in range(KERNEL)[:0:-1]]
            for i in range(steps // tall):
                first = g * steps + i * tall
                here = slice(first, first + tall)
                x0 = acc[0, here, hi]
                conv = w[0] * x0
                for j in range(1, KERNEL):
                    if i:
                        xj = acc[0, first - j * SUB : first - j * SUB + tall, hi]
                    else:
                        xj = jnp.concatenate(old[KERNEL - 1 - j :] + [x0[: tall - j * SUB]], 0)
                    conv += w[j] * xj
                recur = 0.5 * jnp.tanh(0.5 * (acc[1, here, lo] + b0)) + 0.5
                inflow = 0.5 * jnp.tanh(0.5 * (acc[1, here, hi] + b1)) + 0.5
                a = jnp.exp(recur * scale)
                left = 1.0 - a * a
                root = left * lax.rsqrt(jnp.maximum(left, 1e-30))
                acc[0, here, lo] = jax.nn.gelu(acc[0, here, lo])
                acc[1, here, lo] = a
                acc[1, here, hi] = root * inflow * conv

        def step(t, state):
            new = []
            for g in range(games):
                h, p = state[g]
                here = lines(g, t)
                a = acc[1, here, lo]
                h = a * h + acc[1, here, hi]
                p = a * p
                acc[1, here, lo] = p
                acc[1, here, hi] = h
                new.append((h, p))
            return tuple(new)

        zero = jnp.zeros((SUB, LANE), jnp.float32)
        final = lax.fori_loop(0, seg, step, tuple((zero, zero + 1.0) for g in range(games)), unroll=8)
        for g in range(games):
            h, p = final[g]
            run, dec = jnp.zeros((1, LANE), jnp.float32), jnp.ones((1, LANE), jnp.float32)
            for s in range(SUB):
                carry_s[g, 0, s : s + 1, :] = run
                carry_s[g, 1, s : s + 1, :] = dec
                run = p[s : s + 1] * run + h[s : s + 1]
                dec = p[s : s + 1] * dec
            ends[c, z, 2 * g : 2 * g + 1, :] = run
            ends[c, z, 2 * g + 1 : 2 * g + 2, :] = dec
        for d in range(1, zn):

            @pl.when(z + d < zn)
            def _():
                ends_copy(c, d, z, (z + d, x)).start()

    def mix_copy(c):
        return remote(mix.at[c, other], mix_in.at[c], mix_s.at[c], mix_r.at[c], partner)

    def finish(c):
        for d in range(1, zn):

            @pl.when(z >= d)
            def _():
                ends_copy(c, d, z - d, (z - d, x)).wait_recv()

        for g in range(games):
            run = jnp.zeros((1, LANE), jnp.float32)
            for j in range(zn - 1):
                run = jnp.where(j < z, ends[c, j, 2 * g + 1 : 2 * g + 2, :] * run + ends[c, j, 2 * g : 2 * g + 1, :], run)
            enter = carry_s[g, 0] + carry_s[g, 1] * run
            enter = jnp.concatenate([enter, enter], 0)
            for i in range(steps // 16):
                here = slice(g * steps + i * 16, g * steps + (i + 1) * 16)
                value = (acc[1, here, hi] + acc[1, here, lo] * enter) * acc[0, here, lo]
                mix[c, g, i * 16 : (i + 1) * 16, :] = value.astype(jnp.bfloat16)
        mix_copy(c).start()

    def project(j):
        for c in (2 * j, 2 * j + 1):
            mix_copy(c).wait_recv()
        ref = wd_all.at[j, y, 0 : n * rows, :]
        remote(ref, ref, dpeer_s.at[j], dpeer_r.at[j], peer).wait_recv()
        remote(ref, ref, drel_s.at[j], drel_r.at[j], peer).wait_recv()
        own = jnp.concatenate([mix[2 * j, y], mix[2 * j + 1, y]], 1)
        theirs = jnp.concatenate([mix_in[2 * j], mix_in[2 * j + 1]], 1)
        part = min(512, half)

        @pl.loop(0, depth // part)
        def _(f):
            cut = pl.ds(pl.multiple_of(f * part, part), part)
            total = down[:, cut]
            for left, w in ((own, y), (theirs, other)):
                total += lax.dot_general(
                    left, wd_all[j, w, cut, :], (((1,), (1,)), ((), ())), preferred_element_type=jnp.float32
                )
            down[:, cut] = total

    begin(0)
    begin(1)
    swap_feat = remote(emb, raw.at[y], feat_s, feat_r, partner)
    swap_feat.start()
    swap_val = remote(wval, wval_all.at[y], val_s, val_r, partner)
    swap_val.start()
    own_emb.wait()
    last = [raw[y, g, steps - 16 : steps, :].astype(jnp.float32)[16 - SUB :] for g in range(games)]
    tail_buf[...] = jnp.concatenate(last, 0).astype(jnp.bfloat16)

    def tail_copy(i):
        return remote(tail_buf, tails.at[y], tail_s.at[i], tail_r.at[i], at(after, core, y if i == 0 else other))

    @pl.when(z < zn - 1)
    def _():
        for i in range(2):
            tail_copy(i).start()

    own_heads.wait()
    quarter = half // 2

    def head_rows(w, c):
        return heads.at[w, :, pl.ds(pl.multiple_of(c * quarter, quarter), quarter)]

    def relay_heads_wait():
        remote(head_rows(other, core), head_rows(other, core), head_s, head_r, partner).wait_recv()

    swap_heads = remote(head_rows(y, core), head_rows(y, core), head_s, head_r, partner)
    relay_heads = remote(head_rows(other, core), head_rows(other, core), hrel_s, hrel_r, peer)
    first_d = [per + j * ((chunks - 2) * per - reach) // max(items - 1, 1) for j in range(items)]

    @pl.loop(0, chunks + 4)
    def _(k):
        @pl.loop(0, per)
        def _(i):
            slot = k * per + i
            for j in range(items):

                @pl.when(slot == first_d[j])
                def _():
                    dbegin(j)

            @pl.when((i == per - 1) & (k < chunks - 2))
            def _():
                begin(k + 2)

            @pl.when(k < chunks)
            def _():
                pump(k, i + 1)

            @pl.when((k >= 1) & (k <= chunks))
            def _():
                pump(k - 1, per + i + 1)

            for j in range(items):
                t = slot - first_d[j]
                dpump(j, t)
                drelay(j, t - 1)

            @pl.when((k == 2) & (i == per - 1))
            def _():
                prepare()
                swap_heads.start()

            @pl.when((k == 5) & (i == per - 1))
            def _():
                relay_heads_wait()
                relay_heads.start()

            @pl.when((i == per - 1) & (k >= 5) & (k % 2 == 1))
            def _():
                project((k - 5) // 2)

            @pl.when(((i == 0) & (k == 3)) | ((i == per - 1) & (k >= 3) & (k < chunks + 2)))
            def _():
                finish(k - 2 - jnp.where(i == 0, 1, 0))

            @pl.when(((i == 0) & (k >= 3) & (k < chunks + 2)) | ((i == per - 1) & (k == 2)))
            def _():
                product(k - 2)
                scan(k - 2)

    remote(head_rows(other, 1 - core), head_rows(other, 1 - core), hrel_s, hrel_r, peer).wait_recv()
    ref = wval_all.at[other]
    remote(ref, ref, val_s, val_r, partner).wait_recv()
    resid = down[...].astype(jnp.bfloat16)
    full = resid.astype(jnp.float32)
    sumsq = jnp.sum(full * full, -1, keepdims=True)
    row = [wval_all[owner].astype(jnp.float32) for owner in range(yn)]
    row = jnp.concatenate([part[i : i + 1, :] for part in row for i in range(half // LANE)], 1)
    score = jnp.sum(full * row, -1, keepdims=True)
    norm = lax.rsqrt(sumsq / depth + 1e-06)
    logits = sum(
        lax.dot_general(
            resid[:, owner * half : (owner + 1) * half], heads[owner], (((1,), (1,)), ((), ())),
            preferred_element_type=jnp.float32,
        )
        for owner in range(yn)
    )
    logits = logits * norm
    value = jnp.tanh(score * norm)
    top = jnp.max(logits, -1, keepdims=True)
    lse = top + jnp.log(jnp.sum(jnp.exp(logits - top), -1, keepdims=True))
    played = moves[pl.ds(y, 1), :].astype(jnp.float32)
    played = jnp.sum(jnp.where(spread, played, 0.0), -1, keepdims=True)
    column = lax.broadcasted_iota(jnp.int32, logits.shape, 1).astype(jnp.float32)
    picked = jnp.sum(jnp.where(column == played, logits, 0.0), -1, keepdims=True)
    target = outcomes[y].astype(jnp.float32)
    loss = lse - picked + (value - target) ** 2
    loss = jnp.sum(jnp.where(spread, loss, 0.0), 0, keepdims=True)
    value = jnp.sum(jnp.where(spread, value, 0.0), 0, keepdims=True)
    position = z * steps + lax.broadcasted_iota(jnp.int32, (1, steps), 1)
    loss = jnp.where(position < lengths[y], loss, 0.0)
    res[y, 0:1, :] = loss
    res[y, 1:2, :] = value
    swap_res = remote(res.at[y], res.at[y], res_s, res_r, partner)
    swap_res.start()
    ref = res.at[other]
    remote(ref, ref, res_s, res_r, partner).wait_recv()
    for owner in range(yn):
        out[owner : owner + 1, :] = res[owner, 0:1, :]
        out[games + owner : games + owner + 1, :] = res[owner, 1:2, :]

    swap_res.wait_send()
    swap_feat.wait_send()
    swap_val.wait_send()
    swap_heads.wait_send()
    relay_heads.wait_send()

    @pl.when(z < zn - 1)
    def _():
        for i in range(2):
            tail_copy(i).wait_send()

    @pl.loop(0, chunks)
    def _(c):
        ref = w_all.at[c, :, 0 : (n - 1) * rows, :]
        remote(ref, ref, ring_s.at[c], peer_r.at[c], peer).wait_send()
        ref = w_all.at[c, :, 0 : n * rows, :]
        remote(ref, ref, peer_s.at[c], peer_r.at[c], peer).wait_send()
        mix_copy(c).wait_send()
        for d in range(1, zn):

            @pl.when(z + d < zn)
            def _():
                ends_copy(c, d, z, (z + d, x)).wait_send()

    @pl.loop(0, items)
    def _(j):
        ref = wd_all.at[j, y, 0 : (n - 1) * rows, :]
        remote(ref, ref, dring_s.at[j], dpeer_r.at[j], peer).wait_send()
        ref = wd_all.at[j, y, 0 : n * rows, :]
        for sem in (dpeer_s, dpart_s, drel_s):
            remote(ref, ref, sem.at[j], dpeer_r.at[j], peer).wait_send()


def core_block(emb, wb, wd, heads, wval, conv_w, bias, rates, moves, lengths, outcomes):
    games, steps, half = emb.shape
    rows, chans = wd.shape
    yn, zn = lax.axis_size("width"), lax.axis_size("tm")
    n = zn * (lax.axis_size("batch") // 2)
    depth, count = yn * half, games * steps
    labels = heads.shape[0]
    assert games == yn and n % 4 == 0
    chunks, wide = chans // LANE, 2 * LANE
    items, reach = chans // wide, n // 2
    vmem = pl.BlockSpec(memory_space=pltpu.VMEM)
    smem = pl.BlockSpec(memory_space=pltpu.SMEM)
    hbm = pl.BlockSpec(memory_space=pl.ANY)
    dma = pltpu.SemaphoreType.DMA
    f32, b16 = jnp.float32, jnp.bfloat16
    return pl.pallas_call(
        core_kernel,
        in_specs=[hbm] * 4 + [vmem] * 5 + [smem] * 2,
        out_specs=vmem,
        out_shape=jax.ShapeDtypeStruct((2 * games, steps), f32),
        scratch_shapes=[
            pltpu.VMEM((chunks, 2, depth, wide), b16),
            pltpu.VMEM((items, yn, depth, wide), b16),
            pltpu.VMEM((yn, games, steps, half), b16),
            pltpu.VMEM((count + games * SUB, depth), b16),
            pltpu.VMEM((games * SUB, half), b16),
            pltpu.VMEM((yn, games * SUB, half), b16),
            pltpu.VMEM((2, count + games * SUB, wide), f32),
            pltpu.VMEM((games, 2, SUB, LANE), f32),
            pltpu.VMEM((chunks, zn, SUB, LANE), f32),
            pltpu.VMEM((chunks, games, steps, LANE), b16),
            pltpu.VMEM((chunks, steps, LANE), b16),
            pltpu.VMEM((steps, depth), f32),
            pltpu.VMEM((yn, labels, half), b16),
            pltpu.VMEM((yn, half // LANE, LANE), b16),
            pltpu.VMEM((yn, SUB, steps), f32),
            dma((chunks,)), dma((items,)), dma, dma, dma, dma, dma((2,)), dma((2,)), dma, dma, dma, dma, dma, dma,
            dma((chunks,)), dma((chunks, 2, 2, reach)), dma((chunks,)), dma((chunks,)),
            dma((items,)), dma((items, 2, reach)), dma((items,)), dma((items,)),
            dma((items,)), dma((items, n)), dma((items,)), dma((items,)),
            dma((chunks, zn)), dma((chunks, zn)), dma((chunks,)), dma((chunks,)), dma, dma,
        ],
        compiler_params=pltpu.CompilerParams(
            collective_id=0, has_side_effects=True, vmem_limit_bytes=56 * 1024 * 1024
        ),
        cost_estimate=pl.CostEstimate(
            flops=8 * count * chans * depth, bytes_accessed=200_000_000, transcendentals=8 * count * chans
        ),
    )(emb, wb, wd, heads, wval, conv_w, bias, rates, moves, lengths, outcomes)


def shards(
    moves,
    lengths,
    outcomes,
    embedded,
    w_branches,
    conv_w,
    gate_bias,
    rates,
    w_down,
    w_policy,
    w_value,
):
    wval = w_value.reshape(-1, LANE)
    out = core_block(
        embedded, w_branches, w_down, w_policy.T, wval, conv_w, gate_bias, rates.reshape(1, -1), moves, lengths, outcomes
    )
    games = embedded.shape[0]
    return out[:games], out[games:]


def solution(mesh):
    in_specs = (
        P("batch", "tm"),
        P("batch"),
        P("batch"),
        P("batch", "tm", "width"),
        P(None, ("tm", "batch"), "width"),
        P(None, "width"),
        P(None, "width"),
        P("width"),
        P(("tm", "batch"), "width"),
        P("width", None),
        P("width"),
    )
    out_specs = (P("batch", "tm"), P("batch", "tm"))
    return jax.shard_map(shards, mesh=mesh, in_specs=in_specs, out_specs=out_specs, check_vma=False)
```

```python
import jax
import jax.numpy as jnp
from jax import lax
from jax.experimental import pallas as pl
from jax.experimental.pallas import tpu as pltpu
from jax.sharding import PartitionSpec as P

KERNEL = 4
SUB = 8
LANE = 128
MESH = pl.DeviceIdType.MESH
DIRS = (0, 1)
PAIRS = (0, 1)


def core_kernel(
    emb, wb, wd, heads_in, wval, conv_w, bias, rates, moves, lengths, outcomes,
    out,
    w_all, wd_all, raw, feat, tail_buf, tails, acc, carry_s, ends, mix, mix_in, down, heads, wval_all, res,
    loc_w, loc_d, loc_e, loc_h, feat_s, feat_r, tail_s, tail_r, val_s, val_r, head_s, head_r, hrel_s, hrel_r,
    ring_s, ring_r, peer_s, peer_r, dring_s, dring_r, dpeer_s, dpeer_r, dpart_s, dpart_r, drel_s, drel_r,
    ends_s, ends_r, mix_s, mix_r, res_s, res_r,
):
    z, b, y = lax.axis_index("tm"), lax.axis_index("batch"), lax.axis_index("width")
    zn, bn, yn = lax.axis_size("tm"), lax.axis_size("batch"), lax.axis_size("width")
    x, core = b // 2, b % 2
    n = zn * (bn // 2)
    rows, chans = wd.shape
    games, steps, half = emb.shape
    depth = yn * half
    count = games * steps
    seg = steps // SUB
    chunks = chans // LANE
    wide = 2 * LANE
    items = chans // wide
    reach = n // 2
    per = n // 4
    other = yn - 1 - y

    def spot(r):
        cx = r // zn
        cz = r % zn
        return cz + (cx % 2) * (zn - 1 - 2 * cz), cx

    r = x * zn + z + (x % 2) * (zn - 1 - 2 * z)

    def at(place, c=core, w=y):
        return {"tm": place[0], "batch": place[1] * 2 + c, "width": w}

    ahead, behind = at(spot((r + 1) % n)), at(spot((r + n - 1) % n))
    peer = at((z, x), 1 - core)
    partner = at((z, x), core, other)
    after = ((z + 1) % zn, x)
    before = ((z + zn - 1) % zn, x)
    greet = [ahead, behind, peer, partner, at(after), at(after, core, other), at(before), at(before, core, other)]
    greet += [at(((z + d) % zn, x)) for d in range(2, zn - 1)]

    def first_row(chip):
        cz, cx = spot(chip)
        return (cz * bn + cx * 2) * rows

    def block(chip, c):
        return pl.ds(pl.multiple_of(first_row(chip) + c * rows, rows), rows)

    mine = block(r, core)

    def dpiece(j, w, chip):
        cz, cx = spot(chip)
        return wd_all.at[j, w, cz * (bn // 2) + cx, core]

    def remote(src, dst, send, recv, device):
        return pltpu.make_async_remote_copy(
            src_ref=src, dst_ref=dst, send_sem=send, recv_sem=recv, device_id=device, device_id_type=MESH
        )

    def load_chunk(c):
        return [
            pltpu.make_async_copy(
                wb.at[m, :, pl.ds(pl.multiple_of(c * LANE, LANE), LANE)],
                w_all.at[c, m // 2, mine, (m % 2) * LANE : (m % 2 + 1) * LANE],
                loc_w,
            )
            for m in range(4)
        ]

    ends[...] = jnp.zeros_like(ends)
    res[...] = jnp.zeros_like(res)
    wval_all[y] = wval[...]
    barrier = pltpu.get_barrier_semaphore()
    for device in greet:
        pl.semaphore_signal(barrier, inc=1, device_id=device, device_id_type=MESH)

    own_emb = pltpu.make_async_copy(emb, raw.at[y], loc_e)
    own_heads = pltpu.make_async_copy(heads_in, heads.at[y], loc_h)
    for copy in load_chunk(0):
        copy.start()
    own_emb.start()
    for c in range(1, chunks):
        for copy in load_chunk(c):
            copy.start()
    for j in range(items):
        pltpu.make_async_copy(wd.at[:, j * wide : (j + 1) * wide], dpiece(j, y, r), loc_d).start()
    own_heads.start()
    pl.semaphore_wait(barrier, len(greet))
    ref = w_all.at[:, :, 0:rows, :]
    pltpu.make_async_copy(ref, ref, loc_w).wait()
    ref = wd_all.at[:, 0, 0, 0]
    pltpu.make_async_copy(ref, ref, loc_d).wait()

    def chip_of(d, t):
        return (r + n - t) % n if d == 0 else (r + t) % n

    def toward(d):
        return ahead if d == 0 else behind

    def hops(which, d):
        return n - 1 - reach + jnp.where(which == d, 2 * reach + 1 - n, 0)

    def piece(c, p, chip):
        return w_all.at[c, p, block(chip, core), :]

    def hop(c, p, d, t):
        ref = piece(c, p, chip_of(d, t - 1))
        return remote(ref, ref, ring_s, ring_r.at[c % 4, p, d, t - 1], toward(d))

    def landed(c, p, d, t):
        ref = piece(c, p, chip_of(d, t))
        return remote(ref, ref, ring_s, ring_r.at[c % 4, p, d, t - 1], toward(d))

    def share(c, p, chip):
        ref = piece(c, p, chip)
        return remote(ref, ref, peer_s, peer_r.at[c], peer)

    def begin(c):
        for p in PAIRS:
            for d in DIRS:
                hop(c, p, d, 1).start()
        for p in PAIRS:
            share(c, p, r).start()

    def pump(c, t):
        for p, d in ((0, 0), (1, 1), (1, 0), (0, 1)):
            last = reach if p == d else n - 1 - reach

            @pl.when(t <= last)
            def _():
                landed(c, p, d, t).wait_recv()

                @pl.when(t < last)
                def _():
                    hop(c, p, d, t + 1).start()

                share(c, p, chip_of(d, t)).start()

    def dhop(j, d, t):
        ref = dpiece(j, y, chip_of(d, t - 1))
        return remote(ref, ref, dring_s, dring_r.at[j % 2, d, t - 1], toward(d))

    def dlanded(j, d, t):
        ref = dpiece(j, y, chip_of(d, t))
        return remote(ref, ref, dring_s, dring_r.at[j % 2, d, t - 1], toward(d))

    def dspread(j, chip):
        ref = dpiece(j, y, chip)
        remote(ref, ref, dpeer_s, dpeer_r.at[j], peer).start()
        remote(ref, ref, dpart_s, dpart_r.at[j], partner).start()

    def dbegin(j):
        for d in DIRS:
            dhop(j, d, 1).start()
        dspread(j, r)

    def dpump(j, t):
        for d in DIRS:
            last = hops(j % 2, d)

            @pl.when(t <= last)
            def _():
                dlanded(j, d, t).wait_recv()

                @pl.when(t < last)
                def _():
                    dhop(j, d, t + 1).start()

                dspread(j, chip_of(d, t))

    def drelay(j):
        ref = wd_all.at[j, other, :, core]
        remote(ref, ref, dpart_s, dpart_r.at[j], partner).wait_recv()
        remote(ref, ref, drel_s, drel_r.at[j], peer).start()

    row_id = lax.broadcasted_iota(jnp.int32, (steps, steps), 0)
    lane_id = lax.broadcasted_iota(jnp.int32, (steps, steps), 1)
    spread = (row_id % SUB) * seg + row_id // SUB == lane_id

    def prepare():
        ref = raw.at[other]
        remote(ref, ref, feat_s, feat_r, partner).wait_recv()
        turn = jnp.where(spread, 1.0, 0.0).astype(jnp.bfloat16)
        for owner in range(yn):
            for g in range(games):
                feat[g * steps : (g + 1) * steps, owner * half : (owner + 1) * half] = jnp.dot(
                    turn, raw[owner, g], preferred_element_type=jnp.float32
                ).astype(jnp.bfloat16)

        @pl.when(z > 0)
        def _():
            for i in range(2):
                ref = tails.at[y if i == 0 else other]
                remote(ref, ref, tail_s.at[i], tail_r.at[i], peer).wait_recv()
            for owner in range(yn):
                feat[count : count + games * SUB, owner * half : (owner + 1) * half] = tails[owner]

        @pl.when(z == 0)
        def _():
            feat[count : count + games * SUB, :] = jnp.zeros((games * SUB, depth), jnp.bfloat16)

        down[...] = feat[pl.ds(pl.multiple_of(y * steps, steps), steps), :].astype(jnp.float32)

    def product(c):
        ref = w_all.at[c, :, 0 : n * rows, :]
        remote(ref, ref, peer_s, peer_r.at[c], peer).wait_recv()

        @pl.loop(0, 2)
        def _(p):
            acc[c % 2, p] = jnp.dot(feat[...], w_all[c, p], preferred_element_type=jnp.float32)

    lo, hi = slice(0, LANE), slice(LANE, 2 * LANE)

    def lines(g, t):
        return pl.ds(pl.multiple_of(g * steps + t * SUB, SUB), SUB)

    def ends_copy(c, d, source, place):
        ref = ends.at[c, source]
        return remote(ref, ref, ends_s.at[d - 1], ends_r.at[c, d - 1], at(place))

    def scan(c):
        q = c % 2
        cut = pl.ds(pl.multiple_of(c * LANE, LANE), LANE)
        w = [conv_w[k : k + 1, cut] for k in range(KERNEL)]
        b0, b1 = bias[0:1, cut], bias[1:2, cut]
        scale = -8.0 * rates[:, cut]
        row = lax.broadcasted_iota(jnp.int32, (SUB, LANE), 0)
        tall = min(64, steps)

        def earlier(g, j):
            rolled = pltpu.roll(acc[q, 0, lines(g, seg - j), hi], 1, 0)
            first = count + g * SUB + SUB - j
            return jnp.where(row == 0, acc[q, 0, first : first + 1, hi], rolled)

        for g in range(games):
            old = [earlier(g, j) for j in range(KERNEL)[:0:-1]]
            for i in range(steps // tall):
                first = g * steps + i * tall
                here = slice(first, first + tall)
                x0 = acc[q, 0, here, hi]
                conv = w[0] * x0
                for j in range(1, KERNEL):
                    if i:
                        xj = acc[q, 0, first - j * SUB : first - j * SUB + tall, hi]
                    else:
                        xj = jnp.concatenate(old[KERNEL - 1 - j :] + [x0[: tall - j * SUB]], 0)
                    conv += w[j] * xj
                recur = 0.5 * jnp.tanh(0.5 * (acc[q, 1, here, lo] + b0)) + 0.5
                inflow = 0.5 * jnp.tanh(0.5 * (acc[q, 1, here, hi] + b1)) + 0.5
                a = jnp.exp(recur * scale)
                left = 1.0 - a * a
                root = left * lax.rsqrt(jnp.maximum(left, 1e-30))
                acc[q, 0, here, lo] = jax.nn.gelu(acc[q, 0, here, lo])
                acc[q, 1, here, lo] = a
                acc[q, 1, here, hi] = root * inflow * conv

        def step(t, state):
            new = []
            for g in range(games):
                h, p = state[g]
                here = lines(g, t)
                a = acc[q, 1, here, lo]
                h = a * h + acc[q, 1, here, hi]
                p = a * p
                acc[q, 1, here, lo] = p
                acc[q, 1, here, hi] = h
                new.append((h, p))
            return tuple(new)

        zero = jnp.zeros((SUB, LANE), jnp.float32)
        final = lax.fori_loop(0, seg, step, tuple((zero, zero + 1.0) for g in range(games)), unroll=8)
        for g in range(games):
            h, p = final[g]
            run, dec = jnp.zeros((1, LANE), jnp.float32), jnp.ones((1, LANE), jnp.float32)
            for s in range(SUB):
                carry_s[q, g, 0, s : s + 1, :] = run
                carry_s[q, g, 1, s : s + 1, :] = dec
                run = p[s : s + 1] * run + h[s : s + 1]
                dec = p[s : s + 1] * dec
            ends[c, z, 2 * g : 2 * g + 1, :] = run
            ends[c, z, 2 * g + 1 : 2 * g + 2, :] = dec
        for d in range(1, zn):

            @pl.when(z + d < zn)
            def _():
                ends_copy(c, d, z, (z + d, x)).start()

    def mix_copy(c):
        return remote(mix.at[c, other], mix_in.at[c], mix_s, mix_r.at[c], partner)

    def finish(c):
        q = c % 2
        for d in range(1, zn):

            @pl.when(z >= d)
            def _():
                ends_copy(c, d, z - d, (z - d, x)).wait_recv()

        for g in range(games):
            run = jnp.zeros((1, LANE), jnp.float32)
            for j in range(zn - 1):
                run = jnp.where(j < z, ends[c, j, 2 * g + 1 : 2 * g + 2, :] * run + ends[c, j, 2 * g : 2 * g + 1, :], run)
            enter = carry_s[q, g, 0] + carry_s[q, g, 1] * run
            enter = jnp.concatenate([enter, enter], 0)
            for i in range(steps // 16):
                here = slice(g * steps + i * 16, g * steps + (i + 1) * 16)
                value = (acc[q, 1, here, hi] + acc[q, 1, here, lo] * enter) * acc[q, 0, here, lo]
                mix[c, g, i * 16 : (i + 1) * 16, :] = value.astype(jnp.bfloat16)
        mix_copy(c).start()

    def project(j):
        for c in (2 * j, 2 * j + 1):
            mix_copy(c).wait_recv()
        ref = wd_all.at[j, y, :, 0]
        remote(ref, ref, dpeer_s, dpeer_r.at[j], peer).wait_recv()
        remote(ref, ref, drel_s, drel_r.at[j], peer).wait_recv()
        own = jnp.concatenate([mix[2 * j, y], mix[2 * j + 1, y]], 1)
        theirs = jnp.concatenate([mix_in[2 * j], mix_in[2 * j + 1]], 1)
        part = min(512, half)
        chips = part // (2 * rows)

        @pl.loop(0, depth // part)
        def _(f):
            cut = pl.ds(pl.multiple_of(f * part, part), part)
            total = down[:, cut]
            for left, w in ((own, y), (theirs, other)):
                right = wd_all[j, w, pl.ds(f * chips, chips)].reshape(part, wide)
                total += lax.dot_general(
                    left, right, (((1,), (1,)), ((), ())), preferred_element_type=jnp.float32
                )
            down[:, cut] = total

    begin(0)
    begin(1)
    swap_feat = remote(emb, raw.at[y], feat_s, feat_r, partner)
    swap_feat.start()
    swap_val = remote(wval, wval_all.at[y], val_s, val_r, partner)
    swap_val.start()
    own_emb.wait()
    last = [raw[y, g, steps - 16 : steps, :].astype(jnp.float32)[16 - SUB :] for g in range(games)]
    tail_buf[...] = jnp.concatenate(last, 0).astype(jnp.bfloat16)

    def tail_copy(i):
        return remote(tail_buf, tails.at[y], tail_s.at[i], tail_r.at[i], at(after, core, y if i == 0 else other))

    @pl.when(z < zn - 1)
    def _():
        for i in range(2):
            tail_copy(i).start()

    own_heads.wait()
    quarter = half // 2
    final = (chunks + 1) * per - 1

    def head_rows(w, c):
        return heads.at[w, :, pl.ds(pl.multiple_of(c * quarter, quarter), quarter)]

    def relay_heads_wait():
        remote(head_rows(other, core), head_rows(other, core), head_s, head_r, partner).wait_recv()

    swap_heads = remote(head_rows(y, core), head_rows(y, core), head_s, head_r, partner)
    relay_heads = remote(head_rows(other, core), head_rows(other, core), hrel_s, hrel_r, peer)
    @pl.loop(0, chunks + 1)
    def _(k):
        @pl.loop(0, per)
        def _(i):
            slot = k * per + i

            @pl.when((i == per - 1) & (k % 2 == 0) & (k < chunks))
            def _():
                dbegin(k // 2)

            @pl.when((i == per - 1) & (k < chunks - 2))
            def _():
                begin(k + 2)

            @pl.when(k < chunks)
            def _():
                pump(k, i + 1)

            @pl.when(k >= 1)
            def _():
                pump(k - 1, per + i + 1)

                @pl.when(slot < final)
                def _():
                    dpump((slot - per) // reach, (slot - per) % reach + 1)

            @pl.when((slot >= 2 * reach) & (slot % reach == 0))
            def _():
                drelay(slot // reach - 2)

            @pl.when((k == 2) & (i == per - 1))
            def _():
                prepare()
                swap_heads.start()

            @pl.when((k == 5) & (i == per - 1))
            def _():
                relay_heads_wait()
                relay_heads.start()

            @pl.when((i == per - 1) & (k >= 5) & (k % 2 == 1))
            def _():
                project((k - 5) // 2)

            @pl.when(((i == 0) & (k == 3)) | ((i == per - 1) & (k >= 3) & (k < chunks)))
            def _():
                finish(k - 2 - jnp.where(i == 0, 1, 0))

            @pl.when(((i == 0) & (k >= 3)) | ((i == per - 1) & (k == 2)))
            def _():
                product(k - 2)
                scan(k - 2)

    product(chunks - 1)
    scan(chunks - 1)
    dpump(items - 1, reach)
    finish(chunks - 2)
    project(items - 2)
    finish(chunks - 1)
    drelay(items - 1)
    ref = w_all.at[:, :, 0 : (n - 1) * rows, :]
    remote(ref, ref, ring_s, peer_r.at[0], peer).wait_send()
    ref = w_all.at[:, :, 0 : n * rows, :]
    remote(ref, ref, peer_s, peer_r.at[0], peer).wait_send()
    ref = wd_all.at[:, y, 0 : n - 1, 0]
    remote(ref, ref, dring_s, dpeer_r.at[0], peer).wait_send()
    ref = wd_all.at[:, y, :, 0]
    for sem in (dpeer_s, dpart_s, drel_s):
        remote(ref, ref, sem, dpeer_r.at[0], peer).wait_send()
    for d in range(1, zn):

        @pl.when(z + d < zn)
        def _():
            ref = ends.at[:, z]
            remote(ref, ref, ends_s.at[d - 1], ends_r.at[0, d - 1], peer).wait_send()

    project(items - 1)
    remote(head_rows(other, 1 - core), head_rows(other, 1 - core), hrel_s, hrel_r, peer).wait_recv()
    ref = wval_all.at[other]
    remote(ref, ref, val_s, val_r, partner).wait_recv()
    resid = down[...].astype(jnp.bfloat16)
    full = resid.astype(jnp.float32)
    sumsq = jnp.sum(full * full, -1, keepdims=True)
    row = [wval_all[owner].astype(jnp.float32) for owner in range(yn)]
    row = jnp.concatenate([part[i : i + 1, :] for part in row for i in range(half // LANE)], 1)
    score = jnp.sum(full * row, -1, keepdims=True)
    norm = lax.rsqrt(sumsq / depth + 1e-06)
    logits = sum(
        lax.dot_general(
            resid[:, owner * half : (owner + 1) * half], heads[owner], (((1,), (1,)), ((), ())),
            preferred_element_type=jnp.float32,
        )
        for owner in range(yn)
    )
    logits = logits * norm
    value = jnp.tanh(score * norm)
    top = jnp.max(logits, -1, keepdims=True)
    lse = top + jnp.log(jnp.sum(jnp.exp(logits - top), -1, keepdims=True))
    played = moves[pl.ds(y, 1), :].astype(jnp.float32)
    played = jnp.sum(jnp.where(spread, played, 0.0), -1, keepdims=True)
    column = lax.broadcasted_iota(jnp.int32, logits.shape, 1).astype(jnp.float32)
    picked = jnp.sum(jnp.where(column == played, logits, 0.0), -1, keepdims=True)
    target = outcomes[y].astype(jnp.float32)
    loss = lse - picked + (value - target) ** 2
    loss = jnp.sum(jnp.where(spread, loss, 0.0), 0, keepdims=True)
    value = jnp.sum(jnp.where(spread, value, 0.0), 0, keepdims=True)
    position = z * steps + lax.broadcasted_iota(jnp.int32, (1, steps), 1)
    loss = jnp.where(position < lengths[y], loss, 0.0)
    res[y, 0:1, :] = loss
    res[y, 1:2, :] = value
    swap_res = remote(res.at[y], res.at[y], res_s, res_r, partner)
    swap_res.start()
    swap_feat.wait_send()
    swap_val.wait_send()
    swap_heads.wait_send()
    relay_heads.wait_send()

    @pl.when(z < zn - 1)
    def _():
        for i in range(2):
            tail_copy(i).wait_send()

    ref = mix.at[:, other]
    remote(ref, ref, mix_s, mix_r.at[0], partner).wait_send()

    ref = res.at[other]
    remote(ref, ref, res_s, res_r, partner).wait_recv()
    for owner in range(yn):
        out[owner : owner + 1, :] = res[owner, 0:1, :]
        out[games + owner : games + owner + 1, :] = res[owner, 1:2, :]

    swap_res.wait_send()


def core_block(emb, wb, wd, heads, wval, conv_w, bias, rates, moves, lengths, outcomes):
    games, steps, half = emb.shape
    rows, chans = wd.shape
    yn, zn = lax.axis_size("width"), lax.axis_size("tm")
    n = zn * (lax.axis_size("batch") // 2)
    depth, count = yn * half, games * steps
    labels = heads.shape[0]
    assert games == yn and n % 4 == 0
    chunks, wide = chans // LANE, 2 * LANE
    items, reach = chans // wide, n // 2
    vmem = pl.BlockSpec(memory_space=pltpu.VMEM)
    smem = pl.BlockSpec(memory_space=pltpu.SMEM)
    hbm = pl.BlockSpec(memory_space=pl.ANY)
    dma = pltpu.SemaphoreType.DMA
    f32, b16 = jnp.float32, jnp.bfloat16
    return pl.pallas_call(
        core_kernel,
        in_specs=[hbm] * 4 + [vmem] * 5 + [smem] * 2,
        out_specs=vmem,
        out_shape=jax.ShapeDtypeStruct((2 * games, steps), f32),
        scratch_shapes=[
            pltpu.VMEM((chunks, 2, depth, wide), b16),
            pltpu.VMEM((items, yn, n, 2, rows, wide), b16),
            pltpu.VMEM((yn, games, steps, half), b16),
            pltpu.VMEM((count + games * SUB, depth), b16),
            pltpu.VMEM((games * SUB, half), b16),
            pltpu.VMEM((yn, games * SUB, half), b16),
            pltpu.VMEM((2, 2, count + games * SUB, wide), f32),
            pltpu.VMEM((2, games, 2, SUB, LANE), f32),
            pltpu.VMEM((chunks, zn, SUB, LANE), f32),
            pltpu.VMEM((chunks, games, steps, LANE), b16),
            pltpu.VMEM((chunks, steps, LANE), b16),
            pltpu.VMEM((steps, depth), f32),
            pltpu.VMEM((yn, labels, half), b16),
            pltpu.VMEM((yn, half // LANE, LANE), b16),
            pltpu.VMEM((yn, SUB, steps), f32),
            dma, dma, dma, dma, dma, dma, dma((2,)), dma((2,)), dma, dma, dma, dma, dma, dma,
            dma, dma((4, 2, 2, reach)), dma, dma((chunks,)), dma, dma((2, 2, reach)), dma, dma((items,)),
            dma, dma((items,)), dma, dma((items,)),
            dma((zn - 1,)), dma((chunks, zn - 1)), dma, dma((chunks,)), dma, dma,
        ],
        compiler_params=pltpu.CompilerParams(
            collective_id=0, has_side_effects=True, vmem_limit_bytes=56 * 1024 * 1024
        ),
        cost_estimate=pl.CostEstimate(
            flops=8 * count * chans * depth, bytes_accessed=200_000_000, transcendentals=8 * count * chans
        ),
    )(emb, wb, wd, heads, wval, conv_w, bias, rates, moves, lengths, outcomes)


def shards(
    moves,
    lengths,
    outcomes,
    embedded,
    w_branches,
    conv_w,
    gate_bias,
    rates,
    w_down,
    w_policy,
    w_value,
):
    wval = w_value.reshape(-1, LANE)
    out = core_block(
        embedded, w_branches, w_down, w_policy.T, wval, conv_w, gate_bias, rates.reshape(1, -1), moves, lengths, outcomes
    )
    games = embedded.shape[0]
    return out[:games], out[games:]


def solution(mesh):
    in_specs = (
        P("batch", "tm"),
        P("batch"),
        P("batch"),
        P("batch", "tm", "width"),
        P(None, ("tm", "batch"), "width"),
        P(None, "width"),
        P(None, "width"),
        P("width"),
        P(("tm", "batch"), "width"),
        P("width", None),
        P("width"),
    )
    out_specs = (P("batch", "tm"), P("batch", "tm"))
    return jax.shard_map(shards, mesh=mesh, in_specs=in_specs, out_specs=out_specs, check_vma=False)
```
